128 devices in a mesh: gx: 8 (over y, z_lo), gz: 16 (over z_hi, x, core).
Axes of the slice: x: 4, y: 4, z: 4 (z_hi: 2, z_lo: 2; z = z_hi * 2 + z_lo), core: 2. Of those that a mesh axis runs over, the one named last changes fastest.
Arguments:
- sources: float32 [16, 8, 8, 1280, 128], P('gz', 'gx'), may hold values from -6 to 6
- green: float32 [16, 8, 1280, 1280], P('gz', 'gx'), may hold values from -0.2 to 1.2
- probe: float32 [16, 8, 1024, 1280], P('gz', 'gx'), may hold values from -0.0625 to 0.0625
- batch_pick: int32 [8, 23], replicated, may hold values from 0 to 7
- owner_map: int32 [16, 512], P('gz'), may hold values from 0 to 511, each once within a row
Outputs:
- outgoing: float32 [16, 8, 1280, 1024], P('gz', 'gx')
- receiver_data: float32 [16, 2, 512, 1024], P('gz', None, 'gx')
The draws below stay inside these ranges and needn't reach their ends.
Inputs may be any that keep to these rules, and one draw needn't show every extreme that they name: Each row of owner_map holds every receiver once; slot q belongs to the column q // (512 // 8).
All inputs are finite; a program needn't handle non-finite values.
Results may differ from the reference program's by a relative error of at most 0.00013.
Values sent between devices are 32-bit elements; how exact they have to be, the bound alone decides.
No kernel may reach another device: no remote copies, remote signals or barrier semaphores. Data moves between devices by JAX's collectives and lax.ppermute only.
A program may use at most 128 MiB of HBM per device.

```python
import jax
import jax.numpy as jnp
from jax import lax

TRACE = 1280
RECV = 512
SHOTS = 128
SHOTSETS = 8
WINDOW = 8
DIAGS = 23
N_GX = 8
N_GZ = 16


def draw_green(key, part):
    first, second = jax.random.split(key)
    shape = (N_GZ, N_GX, TRACE, TRACE)
    diagonal = jax.random.uniform(first, (N_GZ, N_GX, TRACE), jnp.float32, 0.7, 1.0)
    spread = jax.random.truncated_normal(second, -4.0, 4.0, shape, jnp.float32) * 0.35 / TRACE ** 0.5
    identity = jnp.eye(TRACE, dtype=jnp.float32)
    return spread + diagonal[..., None] * identity


def touch_ends(entries, own_key, low, largest):
    extent = entries.shape
    place = [jax.random.randint(jax.random.fold_in(own_key, axis), (), 0, extent[axis]) for axis in range(len(extent))]
    entries = entries.at[tuple(place)].set(low)
    longest = extent.index(max(extent))
    place[longest] = (place[longest] + 1) % extent[longest]
    return entries.at[tuple(place)].set(largest)


def steps_of(rng, shape, shards, low, top_value):
    gain = 1.0
    for dim, parts in shards:
        steps = jax.random.uniform(jax.random.fold_in(jax.random.fold_in(rng, 6), dim), (parts,), jnp.float32, low / len(shards), top_value / len(shards))
        gain = gain * jnp.repeat(jnp.exp(steps), shape[dim] // parts).reshape((-1,) + (1,) * (len(shape) - 1 - dim))
    return gain


def bell_draw(stream_key, extent, scale, limit, cuts=(), kind=jnp.bfloat16):
    values = scale * jax.random.normal(stream_key, extent, jnp.float32)
    if cuts:
        values = values * steps_of(stream_key, extent, cuts, -0.22, 0.18)
    return jnp.clip(values, -limit, limit).astype(kind)


def setup_inputs(seed: int = 0) -> dict:
    key_list = jax.random.split(jax.random.key(seed), 6)
    return {
        "sources": bell_draw(key_list[0], (N_GZ, N_GX, SHOTSETS, TRACE, SHOTS), 1.0, 6.0, ((0, 16), (1, 8)), jnp.float32),
        "green": draw_green(jax.random.fold_in(key_list[5], 71), 0),
        "probe": bell_draw(key_list[2], (N_GZ, N_GX, 2 * RECV, TRACE), (TRACE * N_GX) ** -0.5, 0.0625, ((0, 16), (1, 8)), jnp.float32),
        "batch_pick": touch_ends(jax.random.randint(key_list[3], (WINDOW, DIAGS), 0, SHOTSETS), jax.random.fold_in(key_list[3], 1), 0, SHOTSETS - 1).astype(jnp.int32),
        "owner_map": jax.vmap(lambda own: jax.random.permutation(own, RECV))(jax.random.split(key_list[4], N_GZ)).reshape((N_GZ, RECV)).astype(jnp.int32),
    }


def reference(sources, green, probe, batch_pick, owner_map):
    columns = WINDOW * SHOTS
    above = [jnp.zeros((TRACE, columns), jnp.float32) for col in range(N_GX)]
    traces_rows = []
    data_rows = []
    for row in range(N_GZ):
        lefter = jnp.zeros((TRACE, columns), jnp.float32)
        current = []
        row_sum = jnp.zeros((2 * RECV, columns), jnp.float32)
        for col in range(N_GX):
            chosen = batch_pick[:, row + col]
            picked = sources[row, col][chosen]
            source = jnp.transpose(picked, (1, 0, 2)).reshape(TRACE, columns)
            inflow = source + 0.5 * (above[col] + lefter)
            result = jnp.dot(green[row, col], inflow, precision=lax.Precision.HIGHEST, preferred_element_type=jnp.float32)
            row_sum = row_sum + jnp.dot(probe[row, col], result, precision=lax.Precision.HIGHEST, preferred_element_type=jnp.float32)
            current.append(result)
            lefter = result
        above = current
        traces_rows.append(jnp.stack(current))
        shaped = row_sum.reshape(2, RECV, columns)
        data_rows.append(jnp.take(shaped, owner_map[row].astype(jnp.int32), axis=1))
    return jnp.stack(traces_rows), jnp.stack(data_rows)
```

```python
import functools

import jax
import jax.numpy as jnp
from jax import lax
from jax.experimental import pallas as pl
from jax.experimental.pallas import tpu as pltpu
from jax.sharding import PartitionSpec as P


UNIT = 32
SKEW = 2
VMEM = pltpu.MemorySpace.VMEM
SMEM = pltpu.MemorySpace.SMEM


def passed_along(value, axis, steps):
    count = lax.axis_size(axis)
    return lax.ppermute(value, axis, [(place, place + steps) for place in range(count - steps)])


def swapped(value, axis):
    count = lax.axis_size(axis)
    return lax.ppermute(value, axis, [(place, place ^ 1) for place in range(count)])


def pick_kernel(picks, sources, theirs, sems):
    count = theirs.shape[0]
    copies = [pltpu.make_async_copy(sources.at[picks[1, place]], theirs.at[place], sems.at[place]) for place in range(count)]
    for copy in copies:
        copy.start()
    for copy in copies:
        copy.wait()


def picked(picks, sources):
    count = picks.shape[1]
    return pl.pallas_call(
        pick_kernel,
        out_shape=pltpu.VMEM((count,) + sources.shape[1:], sources.dtype),
        in_specs=[pl.BlockSpec(memory_space=SMEM), pl.BlockSpec(memory_space=pl.ANY)],
        out_specs=pl.BlockSpec(memory_space=VMEM),
        scratch_shapes=[pltpu.SemaphoreType.DMA((count,))],
        compiler_params=pltpu.CompilerParams(vmem_limit_bytes=4 * 1024 * 1024),
        name="pick",
    )(picks, sources)


def split(x):
    high = x.astype(jnp.bfloat16)
    low = (x - high.astype(jnp.float32)).astype(jnp.bfloat16)
    return high, low


def fill(slot, green, slab_copies, pairs, inputs, rows, slabs, row_sems):
    trace = green.shape[0]
    chunk = rows.shape[1]
    steps = trace // chunk
    shots = slabs.shape[2]

    def row_copy(step):
        place = pl.ds(pl.multiple_of(step * chunk, chunk), chunk)
        return pltpu.make_async_copy(green.at[place], rows.at[step % 2], row_sems.at[step % 2])

    row_copy(0).start()
    for copy in slab_copies:
        copy.start()

    def one_chunk(step, nothing):
        @pl.when(step + 1 < steps)
        def _():
            row_copy(step + 1).start()

        row_copy(step).wait()
        high, low = split(rows[step % 2].T)
        pairs[slot, :, pl.ds(pl.multiple_of(step * chunk, chunk), chunk)] = high
        pairs[slot, :, pl.ds(pl.multiple_of(trace + step * chunk, chunk), chunk)] = low
        return nothing

    lax.fori_loop(0, steps, one_chunk, 0)
    for place, copy in enumerate(slab_copies):
        copy.wait()
        inputs[slot, pl.ds(place * shots, shots), :] = slabs[place].T


def own_kernel(core, picks, green, sources, pairs, inputs, store, rows, slabs, row_sems, slab_sems):
    del store
    copies = [pltpu.make_async_copy(sources.at[picks[0, place]], slabs.at[place], slab_sems.at[place]) for place in range(slabs.shape[0])]
    fill(core[0], green, copies, pairs, inputs, rows, slabs, row_sems)


def other_kernel(core, green, theirs, pairs_in, inputs_in, pairs, inputs, rows, slabs, row_sems, slab_sems):
    del pairs_in, inputs_in
    copies = [pltpu.make_async_copy(theirs.at[place], slabs.at[place], slab_sems.at[place]) for place in range(slabs.shape[0])]
    fill(1 - core[0], green, copies, pairs, inputs, rows, slabs, row_sems)


def fill_scratch(trace, count, shots):
    return [
        pltpu.VMEM((2, 128, trace), jnp.float32),
        pltpu.VMEM((count, trace, shots), jnp.float32),
        pltpu.SemaphoreType.DMA((2,)),
        pltpu.SemaphoreType.DMA((count,)),
    ]


def own_side(core, picks, green, sources):
    trace = green.shape[0]
    count = picks.shape[1]
    shots = sources.shape[2]
    columns = count * shots
    scalar = pl.BlockSpec(memory_space=SMEM)
    anywhere = pl.BlockSpec(memory_space=pl.ANY)
    inside = pl.BlockSpec(memory_space=VMEM)
    return pl.pallas_call(
        own_kernel,
        out_shape=(
            pltpu.VMEM((2, trace, 2 * trace), jnp.bfloat16),
            pltpu.VMEM((2, columns, trace), jnp.float32),
            pltpu.VMEM((2, columns, trace), jnp.float32),
        ),
        in_specs=[scalar, scalar, anywhere, anywhere],
        out_specs=(inside,) * 3,
        scratch_shapes=fill_scratch(trace, count, shots),
        compiler_params=pltpu.CompilerParams(vmem_limit_bytes=12 * 1024 * 1024),
        name="own",
    )(core, picks, green, sources)


def other_side(core, green, theirs, pairs, inputs):
    count, trace, shots = theirs.shape
    scalar = pl.BlockSpec(memory_space=SMEM)
    anywhere = pl.BlockSpec(memory_space=pl.ANY)
    inside = pl.BlockSpec(memory_space=VMEM)
    return pl.pallas_call(
        other_kernel,
        out_shape=(pltpu.VMEM(pairs.shape, pairs.dtype), pltpu.VMEM(inputs.shape, inputs.dtype)),
        in_specs=[scalar, anywhere, anywhere, inside, inside],
        out_specs=(inside,) * 2,
        input_output_aliases={3: 0, 4: 1},
        scratch_shapes=fill_scratch(trace, count, shots),
        compiler_params=pltpu.CompilerParams(vmem_limit_bytes=12 * 1024 * 1024),
        name="other",
    )(core, green, theirs, pairs, inputs)


def sweep_kernel(step, units, base, pairs, inputs, upper, lefter, stored, right, lower, store, above, both):
    del stored
    unit = step - base[0]
    size, trace = upper.shape
    block = 640

    @pl.when(jnp.logical_and(unit >= 0, unit < units))
    def _():
        spot = pl.ds(pl.multiple_of(jnp.clip(unit, 0, units - 1) * size, size), size)
        above[...] = upper[...]

        def one_row(row, nothing):
            high, low = split(inputs[row, spot, :] + 0.5 * (above[...] + lefter[row]))
            both[:size, :] = high
            both[size:, :] = low

            def one_block(number, nothing):
                start = pl.multiple_of(number * block, block)
                contract = (((1,), (0,)), ((), ()))
                most = lax.dot_general(both[...], pairs[row, :, pl.ds(start, block)], contract, preferred_element_type=jnp.float32)
                rest = lax.dot_general(both[:size, :], pairs[row, :, pl.ds(trace + start, block)], contract, preferred_element_type=jnp.float32)
                value = most[:size] + (most[size:] + rest)
                above[:, pl.ds(start, block)] = value
                right[row, :, pl.ds(start, block)] = value
                store[row, spot, pl.ds(start, block)] = value
                return nothing

            return lax.fori_loop(0, trace // block, one_block, nothing)

        lax.fori_loop(0, 2, one_row, 0)
        lower[...] = above[...]


def swept(step, units, base, pairs, inputs, upper, lefter, store):
    inside = pl.BlockSpec(memory_space=VMEM)
    return pl.pallas_call(
        functools.partial(sweep_kernel, step, units),
        out_shape=(
            pltpu.VMEM(lefter.shape, jnp.float32),
            pltpu.VMEM(upper.shape, jnp.float32),
            pltpu.VMEM(store.shape, jnp.float32),
        ),
        in_specs=[pl.BlockSpec(memory_space=SMEM)] + [inside] * 5,
        out_specs=(inside,) * 3,
        input_output_aliases={5: 2},
        scratch_shapes=[pltpu.VMEM(upper.shape, jnp.float32), pltpu.VMEM((2 * upper.shape[0], upper.shape[1]), jnp.bfloat16)],
        compiler_params=pltpu.CompilerParams(vmem_limit_bytes=8 * 1024 * 1024),
        name="sweep",
    )(base, pairs, inputs, upper, lefter, store)


def release_kernel(core, store, own, other, sems):
    copies = (
        pltpu.make_async_copy(store.at[1 - core[0]], other, sems.at[0]),
        pltpu.make_async_copy(store.at[core[0]], own, sems.at[1]),
    )
    for copy in copies:
        copy.start()
    for copy in copies:
        copy.wait()


def released(core, store):
    shape = jax.ShapeDtypeStruct(store.shape[1:], store.dtype)
    anywhere = pl.BlockSpec(memory_space=pl.ANY)
    return pl.pallas_call(
        release_kernel,
        out_shape=(shape, shape),
        in_specs=[pl.BlockSpec(memory_space=SMEM), pl.BlockSpec(memory_space=VMEM)],
        out_specs=(anywhere, anywhere),
        scratch_shapes=[pltpu.SemaphoreType.DMA((2,))],
        compiler_params=pltpu.CompilerParams(vmem_limit_bytes=8 * 1024 * 1024),
        name="release",
    )(core, store)


def order_kernel(*refs):
    gate, places, probe, high, low, whole, sem = refs[:3] + refs[-4:]

    @pl.when(gate[0] > 0)
    def _():
        copy = pltpu.make_async_copy(probe, whole, sem)
        copy.start()
        receivers = places.shape[0]
        slots = lax.broadcasted_iota(jnp.int32, (receivers, receivers), 1)
        chosen = jnp.where(slots == places[...], 1.0, 0.0).astype(jnp.bfloat16)
        copy.wait()
        for component in range(whole.shape[0] // receivers):
            span = pl.ds(component * receivers, receivers)
            first, second = split(whole[span, :])
            high[span, :] = jnp.dot(chosen, first, preferred_element_type=jnp.float32).astype(jnp.bfloat16)
            low[span, :] = jnp.dot(chosen, second, preferred_element_type=jnp.float32).astype(jnp.bfloat16)


def ordered(gate, places, probe, before=None):
    inside = pl.BlockSpec(memory_space=VMEM)
    shape = pltpu.VMEM(probe.shape, jnp.bfloat16)
    more = () if before is None else tuple(before)
    return pl.pallas_call(
        order_kernel,
        out_shape=(shape, shape),
        in_specs=[pl.BlockSpec(memory_space=SMEM), inside, pl.BlockSpec(memory_space=pl.ANY)] + [inside] * len(more),
        out_specs=(inside, inside),
        input_output_aliases={3 + number: number for number in range(len(more))},
        scratch_shapes=[pltpu.VMEM(probe.shape, jnp.float32), pltpu.SemaphoreType.DMA],
        compiler_params=pltpu.CompilerParams(vmem_limit_bytes=16 * 1024 * 1024),
        name="order",
    )(gate, places, probe, *more)


def gather_kernel(traces, high, low, *refs):
    straight, partial_value, turned, sem = refs[-4:]
    columns, _ = traces.shape
    block = 256
    copies = []
    for number in range(columns // block):
        span = pl.ds(number * block, block)
        turned[:, span] = traces[span, :].T
        copies.append(pltpu.make_async_copy(turned.at[:, span], straight.at[:, span], sem.at[number]))
        copies[-1].start()
        first, second = split(turned[:, span])
        half = high.shape[0] // 2

        def one_component(component, nothing, span=span, first=first, second=second):
            rows = pl.ds(pl.multiple_of(component * half, half), half)
            value = jnp.dot(high[rows, :], first, preferred_element_type=jnp.float32)
            value += jnp.dot(high[rows, :], second, preferred_element_type=jnp.float32)
            value += jnp.dot(low[rows, :], first, preferred_element_type=jnp.float32)
            partial_value[:, component, :, span] = value.reshape(partial_value.shape[0], partial_value.shape[2], block)
            return nothing

        for component in range(2):
            one_component(component, 0)
    for copy in copies:
        copy.wait()


def gathered(traces, high, low, owners):
    columns, trace = traces.shape
    inside = pl.BlockSpec(memory_space=VMEM)
    anywhere = pl.BlockSpec(memory_space=pl.ANY)
    return pl.pallas_call(
        gather_kernel,
        out_shape=(
            jax.ShapeDtypeStruct((trace, columns), jnp.float32),
            jax.ShapeDtypeStruct((owners, 2, high.shape[0] // (2 * owners), columns), jnp.float32),
        ),
        in_specs=[inside] * 3,
        out_specs=(anywhere, inside),
        scratch_shapes=[pltpu.VMEM((trace, columns), jnp.float32), pltpu.SemaphoreType.DMA((columns // 256,))],
        compiler_params=pltpu.CompilerParams(vmem_limit_bytes=24 * 1024 * 1024),
        name="gather",
    )(traces, high, low)


def local(sources, green, probe, batch_pick, owner_map):
    column = lax.axis_index("gx")
    row = lax.axis_index("gz")
    columns = lax.axis_size("gx")
    rows = lax.axis_size("gz")
    core = lax.bitwise_and(row, 1)
    chip_diag = lax.shift_right_logical(row, 1) + column
    operator = green[0, 0]
    trace = operator.shape[0]
    window = batch_pick.shape[0]
    half = window // 2
    shots = sources.shape[4]
    units = half * shots // UNIT
    steps = units + SKEW * (columns + rows // 2 - 2)
    receivers = owner_map.shape[1]

    other_operator = swapped(operator, "gz")
    on_diag = lax.dynamic_index_in_dim(batch_pick, row + column, 1, keepdims=False).reshape(2, half)
    picks = jnp.where(core == 0, on_diag, on_diag[::-1])
    theirs = swapped(picked(picks, sources[0, 0]), "gz")
    core_word = core.astype(jnp.int32).reshape(1)
    pairs, inputs, store = own_side(core_word, picks, operator, sources[0, 0])
    pairs, inputs = other_side(core_word, other_operator, theirs, pairs, inputs)

    places = owner_map.reshape(receivers, 1)
    late = (chip_diag < 2).astype(jnp.int32).reshape(1)
    high, low = ordered(1 - late, places, probe[0, 0])

    base = (SKEW * chip_diag).astype(jnp.int32).reshape(1)
    uppers = [jnp.zeros((UNIT, trace), jnp.float32)] * SKEW
    lefters = [jnp.zeros((2, UNIT, trace), jnp.float32)] * SKEW
    for step in range(steps):
        right, lower, store = swept(step, units, base, pairs, inputs, uppers[step], lefters[step], store)
        if step + SKEW < steps:
            lefters.append(passed_along(right, "gx", 1))
            uppers.append(passed_along(lower, "gz", 2))
        if step == steps - 4:
            high, low = ordered(late, places, probe[0, 0], (high, low))

    own_traces, other_traces = released(core_word, store)
    arrived = swapped(other_traces, "gz")
    own_straight, own_partial = gathered(own_traces, high, low, columns)
    own_sums = lax.all_to_all(own_partial, "gx", split_axis=0, concat_axis=0, tiled=True)
    far_straight, far_partial = gathered(arrived, high, low, columns)
    far_sums = lax.all_to_all(far_partial, "gx", split_axis=0, concat_axis=0, tiled=True)
    own_sum = own_sums.sum(axis=0)
    far_sum = far_sums.sum(axis=0)

    def in_order(own, far):
        return jnp.where(core == 0, jnp.concatenate([own, far], -1), jnp.concatenate([far, own], -1))

    return (in_order(own_straight, far_straight)[None, None], in_order(own_sum, far_sum)[None])


def solution(mesh):
    return jax.shard_map(
        local,
        mesh=mesh,
        in_specs=(
            P("gz", "gx", None, None, None),
            P("gz", "gx", None, None),
            P("gz", "gx", None, None),
            P(),
            P("gz", None),
        ),
        out_specs=(P("gz", "gx", None, None), P("gz", None, "gx", None)),
        check_vma=False,
    )
```

```python
import functools

import jax
import jax.numpy as jnp
from jax import lax
from jax.experimental import pallas as pl
from jax.experimental.pallas import tpu as pltpu
from jax.sharding import PartitionSpec as P


UNIT = 32
SKEW = 2
VMEM = pltpu.MemorySpace.VMEM
HBM = pltpu.MemorySpace.HBM
SMEM = pltpu.MemorySpace.SMEM


def passed_along(value, moved, live):
    columns, rows = lax.axis_size("gx"), lax.axis_size("gz")
    across, down = moved
    pairs = []
    for column in range(columns - across):
        for row in range(rows - down):
            if live(row // 2 + column):
                pairs.append((column * rows + row, (column + across) * rows + row + down))
    return lax.ppermute(value, ("gx", "gz"), pairs)


def swapped(value, axis):
    count = lax.axis_size(axis)
    return lax.ppermute(value, axis, [(place, place ^ 1) for place in range(count)])


def pick_kernel(picks, sources, theirs, sems):
    count = theirs.shape[0]
    copies = [pltpu.make_async_copy(sources.at[picks[1, place]], theirs.at[place], sems.at[place]) for place in range(count)]
    for copy in copies:
        copy.start()
    for copy in copies:
        copy.wait()


def picked(picks, sources):
    count = picks.shape[1]
    return pl.pallas_call(
        pick_kernel,
        out_shape=pltpu.VMEM((count,) + sources.shape[1:], sources.dtype),
        in_specs=[pl.BlockSpec(memory_space=SMEM), pl.BlockSpec(memory_space=HBM)],
        out_specs=pl.BlockSpec(memory_space=VMEM),
        scratch_shapes=[pltpu.SemaphoreType.DMA((count,))],
        compiler_params=pltpu.CompilerParams(vmem_limit_bytes=4 * 1024 * 1024),
        name="pick",
    )(picks, sources)


def split(x):
    high = x.astype(jnp.bfloat16)
    low = (x - high.astype(jnp.float32)).astype(jnp.bfloat16)
    return high, low


def fill(slot, green, slab_copies, pairs, inputs, rows, slabs, row_sems):
    trace = green.shape[0]
    chunk = rows.shape[1]
    steps = trace // chunk
    shots = slabs.shape[2]

    def row_copy(step):
        place = pl.ds(pl.multiple_of(step * chunk, chunk), chunk)
        return pltpu.make_async_copy(green.at[place], rows.at[step % 2], row_sems.at[step % 2])

    row_copy(0).start()
    for copy in slab_copies:
        copy.start()

    def one_chunk(step, nothing):
        @pl.when(step + 1 < steps)
        def _():
            row_copy(step + 1).start()

        row_copy(step).wait()
        high, low = split(rows[step % 2].T)
        pairs[slot, :, pl.ds(pl.multiple_of(step * chunk, chunk), chunk)] = high
        pairs[slot, :, pl.ds(pl.multiple_of(trace + step * chunk, chunk), chunk)] = low
        return nothing

    lax.fori_loop(0, steps, one_chunk, 0)
    for place, copy in enumerate(slab_copies):
        copy.wait()
        inputs[slot, pl.ds(place * shots, shots), :] = slabs[place].T


def own_kernel(core, picks, green, sources, pairs, inputs, store, rows, slabs, row_sems, slab_sems):
    del store
    copies = [pltpu.make_async_copy(sources.at[picks[0, place]], slabs.at[place], slab_sems.at[place]) for place in range(slabs.shape[0])]
    fill(core[0], green, copies, pairs, inputs, rows, slabs, row_sems)


def other_kernel(core, green, theirs, pairs_in, inputs_in, pairs, inputs, rows, slabs, row_sems, slab_sems):
    del pairs_in, inputs_in
    copies = [pltpu.make_async_copy(theirs.at[place], slabs.at[place], slab_sems.at[place]) for place in range(slabs.shape[0])]
    fill(1 - core[0], green, copies, pairs, inputs, rows, slabs, row_sems)


def fill_scratch(trace, count, shots):
    return [
        pltpu.VMEM((2, 128, trace), jnp.float32),
        pltpu.VMEM((count, trace, shots), jnp.float32),
        pltpu.SemaphoreType.DMA((2,)),
        pltpu.SemaphoreType.DMA((count,)),
    ]


def own_side(core, picks, green, sources):
    trace = green.shape[0]
    count = picks.shape[1]
    shots = sources.shape[2]
    columns = count * shots
    scalar = pl.BlockSpec(memory_space=SMEM)
    anywhere = pl.BlockSpec(memory_space=HBM)
    inside = pl.BlockSpec(memory_space=VMEM)
    return pl.pallas_call(
        own_kernel,
        out_shape=(
            pltpu.VMEM((2, trace, 2 * trace), jnp.bfloat16),
            pltpu.VMEM((2, columns, trace), jnp.float32),
            pltpu.VMEM((2, columns, trace), jnp.float32),
        ),
        in_specs=[scalar, scalar, anywhere, anywhere],
        out_specs=(inside,) * 3,
        scratch_shapes=fill_scratch(trace, count, shots),
        compiler_params=pltpu.CompilerParams(vmem_limit_bytes=12 * 1024 * 1024),
        name="own",
    )(core, picks, green, sources)


def other_side(core, green, theirs, pairs, inputs):
    count, trace, shots = theirs.shape
    scalar = pl.BlockSpec(memory_space=SMEM)
    anywhere = pl.BlockSpec(memory_space=HBM)
    inside = pl.BlockSpec(memory_space=VMEM)
    return pl.pallas_call(
        other_kernel,
        out_shape=(pltpu.VMEM(pairs.shape, pairs.dtype), pltpu.VMEM(inputs.shape, inputs.dtype)),
        in_specs=[scalar, anywhere, anywhere, inside, inside],
        out_specs=(inside,) * 2,
        input_output_aliases={3: 0, 4: 1},
        scratch_shapes=fill_scratch(trace, count, shots),
        compiler_params=pltpu.CompilerParams(vmem_limit_bytes=12 * 1024 * 1024),
        name="other",
    )(core, green, theirs, pairs, inputs)


def sweep_kernel(step, units, base, pairs, inputs, upper, lefter, stored, right, lower, store, above, both):
    del stored
    unit = step - base[0]
    size, trace = upper.shape
    block = 640

    @pl.when(jnp.logical_and(unit >= 0, unit < units))
    def _():
        spot = pl.ds(pl.multiple_of(jnp.clip(unit, 0, units - 1) * size, size), size)
        above[...] = upper[...]

        def one_row(row, nothing):
            high, low = split(inputs[row, spot, :] + 0.5 * (above[...] + lefter[row]))
            both[:size, :] = high
            both[size:, :] = low

            def one_block(number, nothing):
                start = pl.multiple_of(number * block, block)
                contract = (((1,), (0,)), ((), ()))
                most = lax.dot_general(both[...], pairs[row, :, pl.ds(start, block)], contract, preferred_element_type=jnp.float32)
                rest = lax.dot_general(both[:size, :], pairs[row, :, pl.ds(trace + start, block)], contract, preferred_element_type=jnp.float32)
                value = most[:size] + (most[size:] + rest)
                above[:, pl.ds(start, block)] = value
                right[row, :, pl.ds(start, block)] = value
                store[row, spot, pl.ds(start, block)] = value
                return nothing

            return lax.fori_loop(0, trace // block, one_block, nothing)

        lax.fori_loop(0, 2, one_row, 0)
        lower[...] = above[...]


def swept(step, units, base, pairs, inputs, upper, lefter, store):
    inside = pl.BlockSpec(memory_space=VMEM)
    return pl.pallas_call(
        functools.partial(sweep_kernel, step, units),
        out_shape=(
            pltpu.VMEM(lefter.shape, jnp.float32),
            pltpu.VMEM(upper.shape, jnp.float32),
            pltpu.VMEM(store.shape, jnp.float32),
        ),
        in_specs=[pl.BlockSpec(memory_space=SMEM)] + [inside] * 5,
        out_specs=(inside,) * 3,
        input_output_aliases={5: 2},
        scratch_shapes=[pltpu.VMEM(upper.shape, jnp.float32), pltpu.VMEM((2 * upper.shape[0], upper.shape[1]), jnp.bfloat16)],
        compiler_params=pltpu.CompilerParams(vmem_limit_bytes=8 * 1024 * 1024),
        name="sweep",
    )(base, pairs, inputs, upper, lefter, store)


def release_kernel(core, store, own, other, sems):
    copies = (
        pltpu.make_async_copy(store.at[1 - core[0]], other, sems.at[0]),
        pltpu.make_async_copy(store.at[core[0]], own, sems.at[1]),
    )
    for copy in copies:
        copy.start()
    for copy in copies:
        copy.wait()


def released(core, store):
    shape = pltpu.HBM(store.shape[1:], store.dtype)
    anywhere = pl.BlockSpec(memory_space=HBM)
    return pl.pallas_call(
        release_kernel,
        out_shape=(shape, shape),
        in_specs=[pl.BlockSpec(memory_space=SMEM), pl.BlockSpec(memory_space=VMEM)],
        out_specs=(anywhere, anywhere),
        scratch_shapes=[pltpu.SemaphoreType.DMA((2,))],
        compiler_params=pltpu.CompilerParams(vmem_limit_bytes=8 * 1024 * 1024),
        name="release",
    )(core, store)


def order_kernel(*refs):
    gate, places, probe, high, low, whole, sem = refs[:3] + refs[-4:]

    @pl.when(gate[0] > 0)
    def _():
        copy = pltpu.make_async_copy(probe, whole, sem)
        copy.start()
        receivers = places.shape[1]
        slots = lax.broadcasted_iota(jnp.int32, (receivers, receivers), 0)
        chosen = jnp.where(slots == places[...], 1.0, 0.0).T.astype(jnp.bfloat16)
        copy.wait()
        for component in range(whole.shape[0] // receivers):
            span = pl.ds(component * receivers, receivers)
            first, second = split(whole[span, :])
            high[span, :] = jnp.dot(chosen, first, preferred_element_type=jnp.float32).astype(jnp.bfloat16)
            low[span, :] = jnp.dot(chosen, second, preferred_element_type=jnp.float32).astype(jnp.bfloat16)


def ordered(gate, places, probe, before=None):
    inside = pl.BlockSpec(memory_space=VMEM)
    shape = pltpu.VMEM(probe.shape, jnp.bfloat16)
    more = () if before is None else tuple(before)
    return pl.pallas_call(
        order_kernel,
        out_shape=(shape, shape),
        in_specs=[pl.BlockSpec(memory_space=SMEM), inside, pl.BlockSpec(memory_space=HBM)] + [inside] * len(more),
        out_specs=(inside, inside),
        input_output_aliases={3 + number: number for number in range(len(more))},
        scratch_shapes=[pltpu.VMEM(probe.shape, jnp.float32), pltpu.SemaphoreType.DMA],
        compiler_params=pltpu.CompilerParams(vmem_limit_bytes=16 * 1024 * 1024),
        name="order",
    )(gate, places, probe, *more)


def gather_kernel(traces, high, low, *refs):
    straight, partial_value, turned, sem = refs[-4:]
    columns, _ = traces.shape
    block = 256
    copies = []
    for number in range(columns // block):
        span = pl.ds(number * block, block)
        turned[:, span] = traces[span, :].T
        copies.append(pltpu.make_async_copy(turned.at[:, span], straight.at[:, span], sem.at[number]))
        copies[-1].start()
        first, second = split(turned[:, span])
        half = high.shape[0] // 2

        def one_component(component, nothing, span=span, first=first, second=second):
            rows = pl.ds(pl.multiple_of(component * half, half), half)
            value = jnp.dot(high[rows, :], first, preferred_element_type=jnp.float32)
            value += jnp.dot(high[rows, :], second, preferred_element_type=jnp.float32)
            value += jnp.dot(low[rows, :], first, preferred_element_type=jnp.float32)
            partial_value[:, component, :, span] = value.reshape(partial_value.shape[0], partial_value.shape[2], block)
            return nothing

        for component in range(2):
            one_component(component, 0)
    for copy in copies:
        copy.wait()


def gathered(traces, high, low, owners):
    columns, trace = traces.shape
    inside = pl.BlockSpec(memory_space=VMEM)
    anywhere = pl.BlockSpec(memory_space=HBM)
    return pl.pallas_call(
        gather_kernel,
        out_shape=(
            pltpu.HBM((trace, columns), jnp.float32),
            jax.ShapeDtypeStruct((owners, 2, high.shape[0] // (2 * owners), columns), jnp.float32),
        ),
        in_specs=[inside] * 3,
        out_specs=(anywhere, inside),
        scratch_shapes=[pltpu.VMEM((trace, columns), jnp.float32), pltpu.SemaphoreType.DMA((columns // 256,))],
        compiler_params=pltpu.CompilerParams(vmem_limit_bytes=24 * 1024 * 1024),
        name="gather",
    )(traces, high, low)


def local(sources, green, probe, batch_pick, owner_map):
    column = lax.axis_index("gx")
    row = lax.axis_index("gz")
    columns = lax.axis_size("gx")
    rows = lax.axis_size("gz")
    core = lax.bitwise_and(row, 1)
    chip_diag = lax.shift_right_logical(row, 1) + column
    operator = green[0, 0]
    trace = operator.shape[0]
    window = batch_pick.shape[0]
    half = window // 2
    shots = sources.shape[4]
    units = half * shots // UNIT
    steps = units + SKEW * (columns + rows // 2 - 2)

    here = pltpu.with_memory_space_constraint(sources[0, 0], HBM)
    operator = pltpu.with_memory_space_constraint(operator, HBM)
    probes = pltpu.with_memory_space_constraint(probe[0, 0], HBM)
    other_operator = swapped(operator, "gz")
    on_diag = lax.dynamic_index_in_dim(batch_pick, row + column, 1, keepdims=False).reshape(2, half)
    picks = jnp.where(core == 0, on_diag, on_diag[::-1])
    core_word = core.astype(jnp.int32).reshape(1)
    places = owner_map
    late = (chip_diag < 2).astype(jnp.int32).reshape(1)
    early = 1 - late
    picks, places, late, early, core_word = lax.optimization_barrier((picks, places, late, early, core_word))
    theirs = swapped(picked(picks, here), "gz")
    pairs, inputs, store = own_side(core_word, picks, operator, here)
    high, low = ordered(early, places, probes)
    pairs, inputs = other_side(core_word, other_operator, theirs, pairs, inputs)

    base = (SKEW * chip_diag).astype(jnp.int32).reshape(1)
    uppers = [jnp.zeros((UNIT, trace), jnp.float32)] * SKEW
    lefters = [jnp.zeros((2, UNIT, trace), jnp.float32)] * SKEW
    for step in range(steps):
        right, lower, store = swept(step, units, base, pairs, inputs, uppers[step], lefters[step], store)
        if step + SKEW < steps:
            def live(diag, step=step):
                return 0 <= step - SKEW * diag < units

            lefters.append(passed_along(right, (1, 0), live))
            uppers.append(passed_along(lower, (0, 2), live))
        if step == steps - 4:
            high, low = ordered(late, places, probes, (high, low))

    own_traces, other_traces = released(core_word, store)
    arrived = swapped(other_traces, "gz")
    own_straight, own_partial = gathered(own_traces, high, low, columns)
    own_sums = lax.all_to_all(own_partial, "gx", split_axis=0, concat_axis=0, tiled=True)
    far_straight, far_partial = gathered(arrived, high, low, columns)
    far_sums = lax.all_to_all(far_partial, "gx", split_axis=0, concat_axis=0, tiled=True)
    own_sum = own_sums.sum(axis=0)
    far_sum = far_sums.sum(axis=0)

    def in_order(own, far):
        return jnp.where(core == 0, jnp.concatenate([own, far], -1), jnp.concatenate([far, own], -1))

    return (in_order(own_straight, far_straight)[None, None], in_order(own_sum, far_sum)[None])


def solution(mesh):
    return jax.shard_map(
        local,
        mesh=mesh,
        in_specs=(
            P("gz", "gx", None, None, None),
            P("gz", "gx", None, None),
            P("gz", "gx", None, None),
            P(),
            P("gz", None),
        ),
        out_specs=(P("gz", "gx", None, None), P("gz", None, "gx", None)),
        check_vma=False,
    )
```

```python
import functools

import jax
import jax.numpy as jnp
from jax import lax
from jax.experimental import pallas as pl
from jax.experimental.pallas import tpu as pltpu
from jax.sharding import PartitionSpec as P


UNIT = 32
SKEW = 2
GROUP = 6
VMEM = pltpu.MemorySpace.VMEM
HBM = pltpu.MemorySpace.HBM
SMEM = pltpu.MemorySpace.SMEM


def passed_along(value, moved, live):
    columns, rows = lax.axis_size("gx"), lax.axis_size("gz")
    across, down = moved
    pairs = []
    for column in range(columns - across):
        for row in range(rows - down):
            if live(row // 2 + column):
                pairs.append((column * rows + row, (column + across) * rows + row + down))
    return lax.ppermute(value, ("gx", "gz"), pairs)


def swapped(value, axis):
    count = lax.axis_size(axis)
    return lax.ppermute(value, axis, [(place, place ^ 1) for place in range(count)])


def pick_kernel(picks, sources, theirs, sems):
    count = theirs.shape[0]
    copies = [pltpu.make_async_copy(sources.at[picks[1, place]], theirs.at[place], sems.at[place]) for place in range(count)]
    for copy in copies:
        copy.start()
    for copy in copies:
        copy.wait()


def picked(picks, sources):
    count = picks.shape[1]
    return pl.pallas_call(
        pick_kernel,
        out_shape=pltpu.VMEM((count,) + sources.shape[1:], sources.dtype),
        in_specs=[pl.BlockSpec(memory_space=SMEM), pl.BlockSpec(memory_space=HBM)],
        out_specs=pl.BlockSpec(memory_space=VMEM),
        scratch_shapes=[pltpu.SemaphoreType.DMA((count,))],
        compiler_params=pltpu.CompilerParams(vmem_limit_bytes=4 * 1024 * 1024),
        name="pick",
    )(picks, sources)


def split(x):
    high = x.astype(jnp.bfloat16)
    low = (x - high.astype(jnp.float32)).astype(jnp.bfloat16)
    return high, low


def fill(slot, green, slab_copies, pairs, inputs, rows, slabs, row_sems):
    trace = green.shape[0]
    chunk = rows.shape[1]
    steps = trace // chunk
    shots = slabs.shape[2]

    def row_copy(step):
        place = pl.ds(pl.multiple_of(step * chunk, chunk), chunk)
        return pltpu.make_async_copy(green.at[place], rows.at[step % 2], row_sems.at[step % 2])

    row_copy(0).start()
    for copy in slab_copies:
        copy.start()

    def one_chunk(step, nothing):
        @pl.when(step + 1 < steps)
        def _():
            row_copy(step + 1).start()

        row_copy(step).wait()
        high, low = split(rows[step % 2].T)
        pairs[slot, :, pl.ds(pl.multiple_of(step * chunk, chunk), chunk)] = high
        pairs[slot, :, pl.ds(pl.multiple_of(trace + step * chunk, chunk), chunk)] = low
        return nothing

    lax.fori_loop(0, steps, one_chunk, 0)
    for place, copy in enumerate(slab_copies):
        copy.wait()
        inputs[slot, pl.ds(place * shots, shots), :] = slabs[place].T


def own_kernel(core, picks, green, sources, pairs, inputs, store, rows, slabs, row_sems, slab_sems):
    del store
    copies = [pltpu.make_async_copy(sources.at[picks[0, place]], slabs.at[place], slab_sems.at[place]) for place in range(slabs.shape[0])]
    fill(core[0], green, copies, pairs, inputs, rows, slabs, row_sems)


def other_kernel(core, green, theirs, pairs_in, inputs_in, pairs, inputs, rows, slabs, row_sems, slab_sems):
    del pairs_in, inputs_in
    copies = [pltpu.make_async_copy(theirs.at[place], slabs.at[place], slab_sems.at[place]) for place in range(slabs.shape[0])]
    fill(1 - core[0], green, copies, pairs, inputs, rows, slabs, row_sems)


def fill_scratch(trace, count, shots):
    return [
        pltpu.VMEM((2, 128, trace), jnp.float32),
        pltpu.VMEM((count, trace, shots), jnp.float32),
        pltpu.SemaphoreType.DMA((2,)),
        pltpu.SemaphoreType.DMA((count,)),
    ]


def own_side(core, picks, green, sources):
    trace = green.shape[0]
    count = picks.shape[1]
    shots = sources.shape[2]
    columns = count * shots
    scalar = pl.BlockSpec(memory_space=SMEM)
    anywhere = pl.BlockSpec(memory_space=HBM)
    inside = pl.BlockSpec(memory_space=VMEM)
    return pl.pallas_call(
        own_kernel,
        out_shape=(
            pltpu.VMEM((2, trace, 2 * trace), jnp.bfloat16),
            pltpu.VMEM((2, columns, trace), jnp.float32),
            pltpu.VMEM((2, columns, trace), jnp.float32),
        ),
        in_specs=[scalar, scalar, anywhere, anywhere],
        out_specs=(inside,) * 3,
        scratch_shapes=fill_scratch(trace, count, shots),
        compiler_params=pltpu.CompilerParams(vmem_limit_bytes=12 * 1024 * 1024),
        name="own",
    )(core, picks, green, sources)


def other_side(core, green, theirs, pairs, inputs):
    count, trace, shots = theirs.shape
    scalar = pl.BlockSpec(memory_space=SMEM)
    anywhere = pl.BlockSpec(memory_space=HBM)
    inside = pl.BlockSpec(memory_space=VMEM)
    return pl.pallas_call(
        other_kernel,
        out_shape=(pltpu.VMEM(pairs.shape, pairs.dtype), pltpu.VMEM(inputs.shape, inputs.dtype)),
        in_specs=[scalar, anywhere, anywhere, inside, inside],
        out_specs=(inside,) * 2,
        input_output_aliases={3: 0, 4: 1},
        scratch_shapes=fill_scratch(trace, count, shots),
        compiler_params=pltpu.CompilerParams(vmem_limit_bytes=12 * 1024 * 1024),
        name="other",
    )(core, green, theirs, pairs, inputs)


def sweep_kernel(step, units, base, pairs, inputs, upper, lefter, stored, right, lower, store, above, both):
    del stored
    unit = step - base[0]
    size, trace = upper.shape
    block = 640

    @pl.when(jnp.logical_and(unit >= 0, unit < units))
    def _():
        spot = pl.ds(pl.multiple_of(jnp.clip(unit, 0, units - 1) * size, size), size)
        above[...] = upper[...]

        def one_row(row, nothing):
            high, low = split(inputs[row, spot, :] + 0.5 * (above[...] + lefter[row]))
            both[:size, :] = high
            both[size:, :] = low

            def one_block(number, nothing):
                start = pl.multiple_of(number * block, block)
                contract = (((1,), (0,)), ((), ()))
                most = lax.dot_general(both[...], pairs[row, :, pl.ds(start, block)], contract, preferred_element_type=jnp.float32)
                rest = lax.dot_general(both[:size, :], pairs[row, :, pl.ds(trace + start, block)], contract, preferred_element_type=jnp.float32)
                value = most[:size] + (most[size:] + rest)
                above[:, pl.ds(start, block)] = value
                right[row, :, pl.ds(start, block)] = value
                store[row, spot, pl.ds(start, block)] = value
                return nothing

            return lax.fori_loop(0, trace // block, one_block, nothing)

        lax.fori_loop(0, 2, one_row, 0)
        lower[...] = above[...]


def swept(step, units, base, pairs, inputs, upper, lefter, store):
    inside = pl.BlockSpec(memory_space=VMEM)
    return pl.pallas_call(
        functools.partial(sweep_kernel, step, units),
        out_shape=(
            pltpu.VMEM(lefter.shape, jnp.float32),
            pltpu.VMEM(upper.shape, jnp.float32),
            pltpu.VMEM(store.shape, jnp.float32),
        ),
        in_specs=[pl.BlockSpec(memory_space=SMEM)] + [inside] * 5,
        out_specs=(inside,) * 3,
        input_output_aliases={5: 2},
        scratch_shapes=[pltpu.VMEM(upper.shape, jnp.float32), pltpu.VMEM((2 * upper.shape[0], upper.shape[1]), jnp.bfloat16)],
        compiler_params=pltpu.CompilerParams(vmem_limit_bytes=8 * 1024 * 1024),
        name="sweep",
    )(base, pairs, inputs, upper, lefter, store)


def release_kernel(core, store, own, other, sems):
    copies = (
        pltpu.make_async_copy(store.at[1 - core[0]], other, sems.at[0]),
        pltpu.make_async_copy(store.at[core[0]], own, sems.at[1]),
    )
    for copy in copies:
        copy.start()
    for copy in copies:
        copy.wait()


def released(core, store):
    shape = pltpu.HBM(store.shape[1:], store.dtype)
    anywhere = pl.BlockSpec(memory_space=HBM)
    return pl.pallas_call(
        release_kernel,
        out_shape=(shape, shape),
        in_specs=[pl.BlockSpec(memory_space=SMEM), pl.BlockSpec(memory_space=VMEM)],
        out_specs=(anywhere, anywhere),
        scratch_shapes=[pltpu.SemaphoreType.DMA((2,))],
        compiler_params=pltpu.CompilerParams(vmem_limit_bytes=8 * 1024 * 1024),
        name="release",
    )(core, store)


def order_kernel(*refs):
    gate, places, probe, high, low, whole, sem = refs[:3] + refs[-4:]

    @pl.when(gate[0] > 0)
    def _():
        copy = pltpu.make_async_copy(probe, whole, sem)
        copy.start()
        receivers = places.shape[1]
        slots = lax.broadcasted_iota(jnp.int32, (receivers, receivers), 0)
        chosen = jnp.where(slots == places[...], 1.0, 0.0).T.astype(jnp.bfloat16)
        copy.wait()
        for component in range(whole.shape[0] // receivers):
            span = pl.ds(component * receivers, receivers)
            first, second = split(whole[span, :])
            high[span, :] = jnp.dot(chosen, first, preferred_element_type=jnp.float32).astype(jnp.bfloat16)
            low[span, :] = jnp.dot(chosen, second, preferred_element_type=jnp.float32).astype(jnp.bfloat16)


def ordered(gate, places, probe, before=None):
    inside = pl.BlockSpec(memory_space=VMEM)
    shape = pltpu.VMEM(probe.shape, jnp.bfloat16)
    more = () if before is None else tuple(before)
    return pl.pallas_call(
        order_kernel,
        out_shape=(shape, shape),
        in_specs=[pl.BlockSpec(memory_space=SMEM), inside, pl.BlockSpec(memory_space=HBM)] + [inside] * len(more),
        out_specs=(inside, inside),
        input_output_aliases={3 + number: number for number in range(len(more))},
        scratch_shapes=[pltpu.VMEM(probe.shape, jnp.float32), pltpu.SemaphoreType.DMA],
        compiler_params=pltpu.CompilerParams(vmem_limit_bytes=16 * 1024 * 1024),
        name="order",
    )(gate, places, probe, *more)


def gather_kernel(traces, high, low, *refs):
    straight, partial_value, turned, sem = refs[-4:]
    columns, _ = traces.shape
    block = 256
    copies = []
    for number in range(columns // block):
        span = pl.ds(number * block, block)
        turned[:, span] = traces[span, :].T
        copies.append(pltpu.make_async_copy(turned.at[:, span], straight.at[:, span], sem.at[number]))
        copies[-1].start()
        first, second = split(turned[:, span])
        half = high.shape[0] // 2

        def one_component(component, nothing, span=span, first=first, second=second):
            rows = pl.ds(pl.multiple_of(component * half, half), half)
            value = jnp.dot(high[rows, :], first, preferred_element_type=jnp.float32)
            value += jnp.dot(high[rows, :], second, preferred_element_type=jnp.float32)
            value += jnp.dot(low[rows, :], first, preferred_element_type=jnp.float32)
            partial_value[:, component, :, span] = value.reshape(partial_value.shape[0], partial_value.shape[2], block)
            return nothing

        for component in range(2):
            one_component(component, 0)
    for copy in copies:
        copy.wait()


def gathered(traces, high, low, owners):
    columns, trace = traces.shape
    inside = pl.BlockSpec(memory_space=VMEM)
    anywhere = pl.BlockSpec(memory_space=HBM)
    return pl.pallas_call(
        gather_kernel,
        out_shape=(
            pltpu.HBM((trace, columns), jnp.float32),
            jax.ShapeDtypeStruct((owners, 2, high.shape[0] // (2 * owners), columns), jnp.float32),
        ),
        in_specs=[inside] * 3,
        out_specs=(anywhere, inside),
        scratch_shapes=[pltpu.VMEM((trace, columns), jnp.float32), pltpu.SemaphoreType.DMA((columns // 256,))],
        compiler_params=pltpu.CompilerParams(vmem_limit_bytes=24 * 1024 * 1024),
        name="gather",
    )(traces, high, low)


def local(sources, green, probe, batch_pick, owner_map):
    column = lax.axis_index("gx")
    row = lax.axis_index("gz")
    columns = lax.axis_size("gx")
    rows = lax.axis_size("gz")
    core = lax.bitwise_and(row, 1)
    chip_diag = lax.shift_right_logical(row, 1) + column
    operator = green[0, 0]
    trace = operator.shape[0]
    window = batch_pick.shape[0]
    half = window // 2
    shots = sources.shape[4]
    units = half * shots // UNIT
    steps = units + SKEW * (columns + rows // 2 - 2)

    here = pltpu.with_memory_space_constraint(sources[0, 0], HBM)
    operator = pltpu.with_memory_space_constraint(operator, HBM)
    probes = pltpu.with_memory_space_constraint(probe[0, 0], HBM)
    other_operator = swapped(operator, "gz")
    on_diag = lax.dynamic_index_in_dim(batch_pick, row + column, 1, keepdims=False).reshape(2, half)
    picks = jnp.where(core == 0, on_diag, on_diag[::-1])
    core_word = core.astype(jnp.int32).reshape(1)
    places = owner_map
    late = (chip_diag < 2).astype(jnp.int32).reshape(1)
    early = 1 - late
    base = (SKEW * chip_diag).astype(jnp.int32).reshape(1)
    picks, places, late, early, core_word, base = lax.optimization_barrier((picks, places, late, early, core_word, base))
    for_other = picked(picks, here)
    pairs, inputs, store = own_side(core_word, picks, operator, here)
    theirs = swapped(for_other, "gz")
    high, low = ordered(early, places, probes)
    pairs, inputs = other_side(core_word, other_operator, theirs, pairs, inputs)

    uppers = [jnp.zeros((UNIT, trace), jnp.float32)] * SKEW
    lefters = [jnp.zeros((2, UNIT, trace), jnp.float32)] * SKEW
    for step in range(steps):
        right, lower, store = swept(step, units, base, pairs, inputs, uppers[step], lefters[step], store)
        if step + SKEW < steps:
            first = step - step % GROUP

            def live(diag, first=first):
                return first + GROUP > SKEW * diag > first - units

            lefters.append(passed_along(right, (1, 0), live))
            uppers.append(passed_along(lower, (0, 2), live))
        if step == steps - 4:
            high, low = ordered(late, places, probes, (high, low))

    own_traces, other_traces = released(core_word, store)
    arrived = swapped(other_traces, "gz")
    own_straight, own_partial = gathered(own_traces, high, low, columns)
    own_sums = lax.all_to_all(own_partial, "gx", split_axis=0, concat_axis=0, tiled=True)
    far_straight, far_partial = gathered(arrived, high, low, columns)
    far_sums = lax.all_to_all(far_partial, "gx", split_axis=0, concat_axis=0, tiled=True)
    own_sum = own_sums.sum(axis=0)
    far_sum = far_sums.sum(axis=0)

    def in_order(own, far):
        return jnp.where(core == 0, jnp.concatenate([own, far], -1), jnp.concatenate([far, own], -1))

    return (in_order(own_straight, far_straight)[None, None], in_order(own_sum, far_sum)[None])


def solution(mesh):
    return jax.shard_map(
        local,
        mesh=mesh,
        in_specs=(
            P("gz", "gx", None, None, None),
            P("gz", "gx", None, None),
            P("gz", "gx", None, None),
            P(),
            P("gz", None),
        ),
        out_specs=(P("gz", "gx", None, None), P("gz", None, "gx", None)),
        check_vma=False,
    )
```

```python
import functools

import jax
import jax.numpy as jnp
from jax import lax
from jax.experimental import pallas as pl
from jax.experimental.pallas import tpu as pltpu
from jax.sharding import PartitionSpec as P


UNIT = 32
SKEW = 2
GROUP = 6
VMEM = pltpu.MemorySpace.VMEM
HBM = pltpu.MemorySpace.HBM
SMEM = pltpu.MemorySpace.SMEM


def passed_along(value, moved, live):
    columns, rows = lax.axis_size("gx"), lax.axis_size("gz")
    across, down = moved
    pairs = []
    for column in range(columns - across):
        for row in range(rows - down):
            if live(row // 2 + column):
                pairs.append((column * rows + row, (column + across) * rows + row + down))
    return lax.ppermute(value, ("gx", "gz"), pairs)


def swapped(value, axis):
    count = lax.axis_size(axis)
    return lax.ppermute(value, axis, [(place, place ^ 1) for place in range(count)])


def pick_kernel(picks, sources, theirs, sems):
    count = theirs.shape[0]
    copies = [pltpu.make_async_copy(sources.at[picks[1, place]], theirs.at[place], sems.at[place]) for place in range(count)]
    for copy in copies:
        copy.start()
    for copy in copies:
        copy.wait()


def picked(picks, sources):
    count = picks.shape[1]
    return pl.pallas_call(
        pick_kernel,
        out_shape=pltpu.VMEM((count,) + sources.shape[1:], sources.dtype),
        in_specs=[pl.BlockSpec(memory_space=SMEM), pl.BlockSpec(memory_space=HBM)],
        out_specs=pl.BlockSpec(memory_space=VMEM),
        scratch_shapes=[pltpu.SemaphoreType.DMA((count,))],
        compiler_params=pltpu.CompilerParams(vmem_limit_bytes=4 * 1024 * 1024),
        name="pick",
    )(picks, sources)


def split(x):
    high = x.astype(jnp.bfloat16)
    low = (x - high.astype(jnp.float32)).astype(jnp.bfloat16)
    return high, low


def fill(slot, green, slab_copies, pairs, inputs, rows, slabs, row_sems):
    trace = green.shape[0]
    chunk = rows.shape[1]
    steps = trace // chunk
    shots = slabs.shape[2]

    def row_copy(step):
        place = pl.ds(pl.multiple_of(step * chunk, chunk), chunk)
        return pltpu.make_async_copy(green.at[place], rows.at[step % 2], row_sems.at[step % 2])

    row_copy(0).start()
    for copy in slab_copies:
        copy.start()

    def one_chunk(step, nothing):
        @pl.when(step + 1 < steps)
        def _():
            row_copy(step + 1).start()

        row_copy(step).wait()
        high, low = split(rows[step % 2].T)
        pairs[slot, :, pl.ds(pl.multiple_of(step * chunk, chunk), chunk)] = high
        pairs[slot, :, pl.ds(pl.multiple_of(trace + step * chunk, chunk), chunk)] = low
        return nothing

    lax.fori_loop(0, steps, one_chunk, 0)
    for place, copy in enumerate(slab_copies):
        copy.wait()
        inputs[slot, pl.ds(place * shots, shots), :] = slabs[place].T


def own_kernel(core, picks, green, sources, pairs, inputs, store, rows, slabs, row_sems, slab_sems):
    del store
    copies = [pltpu.make_async_copy(sources.at[picks[0, place]], slabs.at[place], slab_sems.at[place]) for place in range(slabs.shape[0])]
    fill(core[0], green, copies, pairs, inputs, rows, slabs, row_sems)


def other_kernel(core, green, theirs, pairs_in, inputs_in, pairs, inputs, rows, slabs, row_sems, slab_sems):
    del pairs_in, inputs_in
    copies = [pltpu.make_async_copy(theirs.at[place], slabs.at[place], slab_sems.at[place]) for place in range(slabs.shape[0])]
    fill(1 - core[0], green, copies, pairs, inputs, rows, slabs, row_sems)


def fill_scratch(trace, count, shots):
    return [
        pltpu.VMEM((2, 128, trace), jnp.float32),
        pltpu.VMEM((count, trace, shots), jnp.float32),
        pltpu.SemaphoreType.DMA((2,)),
        pltpu.SemaphoreType.DMA((count,)),
    ]


def own_side(core, picks, green, sources):
    trace = green.shape[0]
    count = picks.shape[1]
    shots = sources.shape[2]
    columns = count * shots
    scalar = pl.BlockSpec(memory_space=SMEM)
    anywhere = pl.BlockSpec(memory_space=HBM)
    inside = pl.BlockSpec(memory_space=VMEM)
    return pl.pallas_call(
        own_kernel,
        out_shape=(
            pltpu.VMEM((2, trace, 2 * trace), jnp.bfloat16),
            pltpu.VMEM((2, columns, trace), jnp.float32),
            pltpu.VMEM((2, columns, trace), jnp.float32),
        ),
        in_specs=[scalar, scalar, anywhere, anywhere],
        out_specs=(inside,) * 3,
        scratch_shapes=fill_scratch(trace, count, shots),
        compiler_params=pltpu.CompilerParams(vmem_limit_bytes=12 * 1024 * 1024),
        name="own",
    )(core, picks, green, sources)


def other_side(core, green, theirs, pairs, inputs):
    count, trace, shots = theirs.shape
    scalar = pl.BlockSpec(memory_space=SMEM)
    anywhere = pl.BlockSpec(memory_space=HBM)
    inside = pl.BlockSpec(memory_space=VMEM)
    return pl.pallas_call(
        other_kernel,
        out_shape=(pltpu.VMEM(pairs.shape, pairs.dtype), pltpu.VMEM(inputs.shape, inputs.dtype)),
        in_specs=[scalar, anywhere, anywhere, inside, inside],
        out_specs=(inside,) * 2,
        input_output_aliases={3: 0, 4: 1},
        scratch_shapes=fill_scratch(trace, count, shots),
        compiler_params=pltpu.CompilerParams(vmem_limit_bytes=12 * 1024 * 1024),
        name="other",
    )(core, green, theirs, pairs, inputs)


def sweep_kernel(step, units, base, pairs, inputs, upper, lefter, stored, right, lower, store, above, both):
    del stored
    unit = step - base[0]
    size, trace = upper.shape
    block = 640

    @pl.when(jnp.logical_and(unit >= 0, unit < units))
    def _():
        spot = pl.ds(pl.multiple_of(jnp.clip(unit, 0, units - 1) * size, size), size)
        above[...] = upper[...]

        def one_row(row, nothing):
            high, low = split(inputs[row, spot, :] + 0.5 * (above[...] + lefter[row]))
            both[:size, :] = high
            both[size:, :] = low

            def one_block(number, nothing):
                start = pl.multiple_of(number * block, block)
                contract = (((1,), (0,)), ((), ()))
                most = lax.dot_general(both[...], pairs[row, :, pl.ds(start, block)], contract, preferred_element_type=jnp.float32)
                rest = lax.dot_general(both[:size, :], pairs[row, :, pl.ds(trace + start, block)], contract, preferred_element_type=jnp.float32)
                value = most[:size] + (most[size:] + rest)
                above[:, pl.ds(start, block)] = value
                right[row, :, pl.ds(start, block)] = value
                store[row, spot, pl.ds(start, block)] = value
                return nothing

            return lax.fori_loop(0, trace // block, one_block, nothing)

        lax.fori_loop(0, 2, one_row, 0)
        lower[...] = above[...]


def swept(step, units, base, pairs, inputs, upper, lefter, store):
    inside = pl.BlockSpec(memory_space=VMEM)
    return pl.pallas_call(
        functools.partial(sweep_kernel, step, units),
        out_shape=(
            pltpu.VMEM(lefter.shape, jnp.float32),
            pltpu.VMEM(upper.shape, jnp.float32),
            pltpu.VMEM(store.shape, jnp.float32),
        ),
        in_specs=[pl.BlockSpec(memory_space=SMEM)] + [inside] * 5,
        out_specs=(inside,) * 3,
        input_output_aliases={5: 2},
        scratch_shapes=[pltpu.VMEM(upper.shape, jnp.float32), pltpu.VMEM((2 * upper.shape[0], upper.shape[1]), jnp.bfloat16)],
        compiler_params=pltpu.CompilerParams(vmem_limit_bytes=8 * 1024 * 1024),
        name="sweep",
    )(base, pairs, inputs, upper, lefter, store)


def release_kernel(start, core, store, own, other, sems):
    span = pl.ds(start, own.shape[0])
    copies = (
        pltpu.make_async_copy(store.at[1 - core[0], span], other, sems.at[0]),
        pltpu.make_async_copy(store.at[core[0], span], own, sems.at[1]),
    )
    for copy in copies:
        copy.start()
    for copy in copies:
        copy.wait()


def released(start, size, core, store):
    shape = pltpu.HBM((size, store.shape[2]), store.dtype)
    anywhere = pl.BlockSpec(memory_space=HBM)
    return pl.pallas_call(
        functools.partial(release_kernel, start),
        out_shape=(shape, shape),
        in_specs=[pl.BlockSpec(memory_space=SMEM), pl.BlockSpec(memory_space=VMEM)],
        out_specs=(anywhere, anywhere),
        scratch_shapes=[pltpu.SemaphoreType.DMA((2,))],
        compiler_params=pltpu.CompilerParams(vmem_limit_bytes=8 * 1024 * 1024),
        name="release",
    )(core, store)


def order_kernel(*refs):
    gate, places, probe, high, low, whole, sem = refs[:3] + refs[-4:]

    @pl.when(gate[0] > 0)
    def _():
        copy = pltpu.make_async_copy(probe, whole, sem)
        copy.start()
        receivers = places.shape[1]
        slots = lax.broadcasted_iota(jnp.int32, (receivers, receivers), 0)
        chosen = jnp.where(slots == places[...], 1.0, 0.0).T.astype(jnp.bfloat16)
        copy.wait()
        for component in range(whole.shape[0] // receivers):
            span = pl.ds(component * receivers, receivers)
            first, second = split(whole[span, :])
            high[span, :] = jnp.dot(chosen, first, preferred_element_type=jnp.float32).astype(jnp.bfloat16)
            low[span, :] = jnp.dot(chosen, second, preferred_element_type=jnp.float32).astype(jnp.bfloat16)


def ordered(gate, places, probe, before=None):
    inside = pl.BlockSpec(memory_space=VMEM)
    shape = pltpu.VMEM(probe.shape, jnp.bfloat16)
    more = () if before is None else tuple(before)
    return pl.pallas_call(
        order_kernel,
        out_shape=(shape, shape),
        in_specs=[pl.BlockSpec(memory_space=SMEM), inside, pl.BlockSpec(memory_space=HBM)] + [inside] * len(more),
        out_specs=(inside, inside),
        input_output_aliases={3 + number: number for number in range(len(more))},
        scratch_shapes=[pltpu.VMEM(probe.shape, jnp.float32), pltpu.SemaphoreType.DMA],
        compiler_params=pltpu.CompilerParams(vmem_limit_bytes=16 * 1024 * 1024),
        name="order",
    )(gate, places, probe, *more)


def gather_kernel(start, aliased, core, own, arrived, high, low, *refs):
    straight, partial_value, loaded, turned, values, in_sems, out_sems, value_sem = refs[aliased:]
    size = own.shape[0]
    half = straight.shape[1] // 2
    pieces = (own, arrived)
    sides = (core[0], 1 - core[0])
    incoming = [pltpu.make_async_copy(piece, loaded.at[number], in_sems.at[number]) for number, piece in enumerate(pieces)]
    for copy in incoming:
        copy.start()
    outgoing = []
    for number, side in enumerate(sides):
        incoming[number].wait()
        span = pl.ds(number * size, size)
        turned[:, span] = loaded[number].T
        place = pl.ds(pl.multiple_of(side * half + start, size), size)
        outgoing.append(pltpu.make_async_copy(turned.at[:, span], straight.at[:, place], out_sems.at[number]))
        outgoing[-1].start()
        first, second = split(turned[:, span])
        receivers = high.shape[0] // 2
        for component in range(2):
            rows = pl.ds(component * receivers, receivers)
            value = jnp.dot(high[rows, :], first, preferred_element_type=jnp.float32)
            value += jnp.dot(high[rows, :], second, preferred_element_type=jnp.float32)
            value += jnp.dot(low[rows, :], first, preferred_element_type=jnp.float32)
            values[:, component, :, span] = value.reshape(values.shape[0], values.shape[2], size)
    last = pltpu.make_async_copy(values, partial_value, value_sem)
    last.start()
    for copy in outgoing:
        copy.wait()
    last.wait()


def gathered(start, core, own, arrived, high, low, owners, columns, straight=None):
    size, trace = own.shape
    inside = pl.BlockSpec(memory_space=VMEM)
    anywhere = pl.BlockSpec(memory_space=HBM)
    more = () if straight is None else (straight,)
    shape = (owners, 2, high.shape[0] // (2 * owners), 2 * size)
    return pl.pallas_call(
        functools.partial(gather_kernel, start, len(more)),
        out_shape=(pltpu.HBM((trace, columns), jnp.float32), pltpu.HBM(shape, jnp.float32)),
        in_specs=[pl.BlockSpec(memory_space=SMEM), anywhere, anywhere, inside, inside] + [anywhere] * len(more),
        out_specs=(anywhere, anywhere),
        input_output_aliases={5 + number: number for number in range(len(more))},
        scratch_shapes=[
            pltpu.VMEM((2, size, trace), jnp.float32),
            pltpu.VMEM((trace, 2 * size), jnp.float32),
            pltpu.VMEM(shape, jnp.float32),
            pltpu.SemaphoreType.DMA((2,)),
            pltpu.SemaphoreType.DMA((2,)),
            pltpu.SemaphoreType.DMA,
        ],
        compiler_params=pltpu.CompilerParams(vmem_limit_bytes=18 * 1024 * 1024),
        name="gather",
    )(core, own, arrived, high, low, *more)


def local(sources, green, probe, batch_pick, owner_map):
    column = lax.axis_index("gx")
    row = lax.axis_index("gz")
    columns = lax.axis_size("gx")
    rows = lax.axis_size("gz")
    core = lax.bitwise_and(row, 1)
    chip_diag = lax.shift_right_logical(row, 1) + column
    operator = green[0, 0]
    trace = operator.shape[0]
    window = batch_pick.shape[0]
    half = window // 2
    shots = sources.shape[4]
    units = half * shots // UNIT
    steps = units + SKEW * (columns + rows // 2 - 2)
    size = half * shots // 2

    here = pltpu.with_memory_space_constraint(sources[0, 0], HBM)
    operator = pltpu.with_memory_space_constraint(operator, HBM)
    probes = pltpu.with_memory_space_constraint(probe[0, 0], HBM)
    other_operator = swapped(operator, "gz")
    on_diag = lax.dynamic_index_in_dim(batch_pick, row + column, 1, keepdims=False).reshape(2, half)
    picks = jnp.where(core == 0, on_diag, on_diag[::-1])
    core_word = core.astype(jnp.int32).reshape(1)
    places = owner_map
    late = (chip_diag < 2).astype(jnp.int32).reshape(1)
    early = 1 - late
    base = (SKEW * chip_diag).astype(jnp.int32).reshape(1)
    picks, places, late, early, core_word, base = lax.optimization_barrier((picks, places, late, early, core_word, base))
    for_other = picked(picks, here)
    pairs, inputs, store = own_side(core_word, picks, operator, here)
    theirs = swapped(for_other, "gz")
    high, low = ordered(early, places, probes)
    pairs, inputs = other_side(core_word, other_operator, theirs, pairs, inputs)

    uppers = [jnp.zeros((UNIT, trace), jnp.float32)] * SKEW
    lefters = [jnp.zeros((2, UNIT, trace), jnp.float32)] * SKEW
    for step in range(steps):
        right, lower, store = swept(step, units, base, pairs, inputs, uppers[step], lefters[step], store)
        if step + SKEW < steps:
            first = step - step % GROUP

            def live(diag, first=first):
                return first + GROUP > SKEW * diag > first - units

            lefters.append(passed_along(right, (1, 0), live))
            uppers.append(passed_along(lower, (0, 2), live))
        if step == steps - 16:
            high, low = ordered(late, places, probes, (high, low))
        if step == steps - 8:
            own_part, other_part = released(0, size, core_word, store)
            base, other_part = lax.optimization_barrier((base, other_part))
            arrived = swapped(other_part, "gz")
            straight, partial_value = gathered(0, core_word, own_part, arrived, high, low, columns, window * shots)

    own_part, other_part = released(size, size, core_word, store)
    arrived = swapped(other_part, "gz")
    first_sums = lax.all_to_all(partial_value, "gx", split_axis=0, concat_axis=0, tiled=True)
    first_sum = first_sums.sum(axis=0)
    straight, partial_value = gathered(size, core_word, own_part, arrived, high, low, columns, window * shots, straight)
    second_sum = lax.all_to_all(partial_value, "gx", split_axis=0, concat_axis=0, tiled=True).sum(axis=0)
    own_sum = jnp.concatenate([first_sum[..., :size], second_sum[..., :size]], -1)
    far_sum = jnp.concatenate([first_sum[..., size:], second_sum[..., size:]], -1)
    total = jnp.where(core == 0, jnp.concatenate([own_sum, far_sum], -1), jnp.concatenate([far_sum, own_sum], -1))
    return (straight[None, None], total[None])


def solution(mesh):
    return jax.shard_map(
        local,
        mesh=mesh,
        in_specs=(
            P("gz", "gx", None, None, None),
            P("gz", "gx", None, None),
            P("gz", "gx", None, None),
            P(),
            P("gz", None),
        ),
        out_specs=(P("gz", "gx", None, None), P("gz", None, "gx", None)),
        check_vma=False,
    )
```

```python
import functools

import jax
import jax.numpy as jnp
from jax import lax
from jax.experimental import pallas as pl
from jax.experimental.pallas import tpu as pltpu
from jax.sharding import PartitionSpec as P


UNIT = 32
SKEW = 2
BOUNDS = (0, 6, 12, 16, 20, 24, 30, 36, 42)
VMEM = pltpu.MemorySpace.VMEM
HBM = pltpu.MemorySpace.HBM
SMEM = pltpu.MemorySpace.SMEM


def passed_along(value, moved, live):
    columns, rows = lax.axis_size("gx"), lax.axis_size("gz")
    across, down = moved
    pairs = []
    for column in range(columns - across):
        for row in range(rows - down):
            if live(row // 2 + column):
                pairs.append((column * rows + row, (column + across) * rows + row + down))
    return lax.ppermute(value, ("gx", "gz"), pairs)


def swapped(value, axis):
    count = lax.axis_size(axis)
    return lax.ppermute(value, axis, [(place, place ^ 1) for place in range(count)])


def pick_kernel(picks, sources, theirs, sems):
    count = theirs.shape[0]
    copies = [pltpu.make_async_copy(sources.at[picks[1, place]], theirs.at[place], sems.at[place]) for place in range(count)]
    for copy in copies:
        copy.start()
    for copy in copies:
        copy.wait()


def picked(picks, sources):
    count = picks.shape[1]
    return pl.pallas_call(
        pick_kernel,
        out_shape=pltpu.VMEM((count,) + sources.shape[1:], sources.dtype),
        in_specs=[pl.BlockSpec(memory_space=SMEM), pl.BlockSpec(memory_space=HBM)],
        out_specs=pl.BlockSpec(memory_space=VMEM),
        scratch_shapes=[pltpu.SemaphoreType.DMA((count,))],
        compiler_params=pltpu.CompilerParams(vmem_limit_bytes=4 * 1024 * 1024),
        name="pick",
    )(picks, sources)


def split(x):
    high = x.astype(jnp.bfloat16)
    low = (x - high.astype(jnp.float32)).astype(jnp.bfloat16)
    return high, low


def fill(slot, green, slab_copies, pairs, inputs, rows, slabs, row_sems):
    trace = green.shape[0]
    chunk = rows.shape[1]
    steps = trace // chunk
    shots = slabs.shape[2]

    def row_copy(step):
        place = pl.ds(pl.multiple_of(step * chunk, chunk), chunk)
        return pltpu.make_async_copy(green.at[place], rows.at[step % 2], row_sems.at[step % 2])

    row_copy(0).start()
    for copy in slab_copies:
        copy.start()

    def one_chunk(step, nothing):
        @pl.when(step + 1 < steps)
        def _():
            row_copy(step + 1).start()

        row_copy(step).wait()
        high, low = split(rows[step % 2].T)
        pairs[slot, :, pl.ds(pl.multiple_of(step * chunk, chunk), chunk)] = high
        pairs[slot, :, pl.ds(pl.multiple_of(trace + step * chunk, chunk), chunk)] = low
        return nothing

    lax.fori_loop(0, steps, one_chunk, 0)
    for place, copy in enumerate(slab_copies):
        copy.wait()
        inputs[slot, pl.ds(place * shots, shots), :] = slabs[place].T


def own_kernel(core, picks, green, sources, pairs, inputs, store, rows, slabs, row_sems, slab_sems):
    del store
    copies = [pltpu.make_async_copy(sources.at[picks[0, place]], slabs.at[place], slab_sems.at[place]) for place in range(slabs.shape[0])]
    fill(core[0], green, copies, pairs, inputs, rows, slabs, row_sems)


def other_kernel(core, green, theirs, pairs_in, inputs_in, pairs, inputs, rows, slabs, row_sems, slab_sems):
    del pairs_in, inputs_in
    copies = [pltpu.make_async_copy(theirs.at[place], slabs.at[place], slab_sems.at[place]) for place in range(slabs.shape[0])]
    fill(1 - core[0], green, copies, pairs, inputs, rows, slabs, row_sems)


def fill_scratch(trace, count, shots):
    return [
        pltpu.VMEM((2, 128, trace), jnp.float32),
        pltpu.VMEM((count, trace, shots), jnp.float32),
        pltpu.SemaphoreType.DMA((2,)),
        pltpu.SemaphoreType.DMA((count,)),
    ]


def own_side(core, picks, green, sources):
    trace = green.shape[0]
    count = picks.shape[1]
    shots = sources.shape[2]
    columns = count * shots
    scalar = pl.BlockSpec(memory_space=SMEM)
    anywhere = pl.BlockSpec(memory_space=HBM)
    inside = pl.BlockSpec(memory_space=VMEM)
    return pl.pallas_call(
        own_kernel,
        out_shape=(
            pltpu.VMEM((2, trace, 2 * trace), jnp.bfloat16),
            pltpu.VMEM((2, columns, trace), jnp.float32),
            pltpu.VMEM((2, columns, trace), jnp.float32),
        ),
        in_specs=[scalar, scalar, anywhere, anywhere],
        out_specs=(inside,) * 3,
        scratch_shapes=fill_scratch(trace, count, shots),
        compiler_params=pltpu.CompilerParams(vmem_limit_bytes=12 * 1024 * 1024),
        name="own",
    )(core, picks, green, sources)


def other_side(core, green, theirs, pairs, inputs):
    count, trace, shots = theirs.shape
    scalar = pl.BlockSpec(memory_space=SMEM)
    anywhere = pl.BlockSpec(memory_space=HBM)
    inside = pl.BlockSpec(memory_space=VMEM)
    return pl.pallas_call(
        other_kernel,
        out_shape=(pltpu.VMEM(pairs.shape, pairs.dtype), pltpu.VMEM(inputs.shape, inputs.dtype)),
        in_specs=[scalar, anywhere, anywhere, inside, inside],
        out_specs=(inside,) * 2,
        input_output_aliases={3: 0, 4: 1},
        scratch_shapes=fill_scratch(trace, count, shots),
        compiler_params=pltpu.CompilerParams(vmem_limit_bytes=12 * 1024 * 1024),
        name="other",
    )(core, green, theirs, pairs, inputs)


def sweep_kernel(step, units, base, pairs, inputs, upper, lefter, stored, right, lower, store, above, both):
    del stored
    unit = step - base[0]
    size, trace = upper.shape
    block = 640

    @pl.when(jnp.logical_and(unit >= 0, unit < units))
    def _():
        spot = pl.ds(pl.multiple_of(jnp.clip(unit, 0, units - 1) * size, size), size)
        above[...] = upper[...]

        def one_row(row, nothing):
            high, low = split(inputs[row, spot, :] + 0.5 * (above[...] + lefter[row]))
            both[:size, :] = high
            both[size:, :] = low

            def one_block(number, nothing):
                start = pl.multiple_of(number * block, block)
                contract = (((1,), (0,)), ((), ()))
                most = lax.dot_general(both[...], pairs[row, :, pl.ds(start, block)], contract, preferred_element_type=jnp.float32)
                rest = lax.dot_general(both[:size, :], pairs[row, :, pl.ds(trace + start, block)], contract, preferred_element_type=jnp.float32)
                value = most[:size] + (most[size:] + rest)
                above[:, pl.ds(start, block)] = value
                right[row, :, pl.ds(start, block)] = value
                store[row, spot, pl.ds(start, block)] = value
                return nothing

            return lax.fori_loop(0, trace // block, one_block, nothing)

        lax.fori_loop(0, 2, one_row, 0)
        lower[...] = above[...]


def swept(step, units, base, pairs, inputs, upper, lefter, store):
    inside = pl.BlockSpec(memory_space=VMEM)
    return pl.pallas_call(
        functools.partial(sweep_kernel, step, units),
        out_shape=(
            pltpu.VMEM(lefter.shape, jnp.float32),
            pltpu.VMEM(upper.shape, jnp.float32),
            pltpu.VMEM(store.shape, jnp.float32),
        ),
        in_specs=[pl.BlockSpec(memory_space=SMEM)] + [inside] * 5,
        out_specs=(inside,) * 3,
        input_output_aliases={5: 2},
        scratch_shapes=[pltpu.VMEM(upper.shape, jnp.float32), pltpu.VMEM((2 * upper.shape[0], upper.shape[1]), jnp.bfloat16)],
        compiler_params=pltpu.CompilerParams(vmem_limit_bytes=8 * 1024 * 1024),
        name="sweep",
    )(base, pairs, inputs, upper, lefter, store)


def release_kernel(start, core, store, own, other, sems):
    span = pl.ds(start, own.shape[0])
    copies = (
        pltpu.make_async_copy(store.at[1 - core[0], span], other, sems.at[0]),
        pltpu.make_async_copy(store.at[core[0], span], own, sems.at[1]),
    )
    for copy in copies:
        copy.start()
    for copy in copies:
        copy.wait()


def released(start, size, core, store):
    shape = pltpu.HBM((size, store.shape[2]), store.dtype)
    anywhere = pl.BlockSpec(memory_space=HBM)
    return pl.pallas_call(
        functools.partial(release_kernel, start),
        out_shape=(shape, shape),
        in_specs=[pl.BlockSpec(memory_space=SMEM), pl.BlockSpec(memory_space=VMEM)],
        out_specs=(anywhere, anywhere),
        scratch_shapes=[pltpu.SemaphoreType.DMA((2,))],
        compiler_params=pltpu.CompilerParams(vmem_limit_bytes=8 * 1024 * 1024),
        name="release",
    )(core, store)


def order_kernel(*refs):
    gate, places, probe, high, low, whole, sem = refs[:3] + refs[-4:]

    @pl.when(gate[0] > 0)
    def _():
        copy = pltpu.make_async_copy(probe, whole, sem)
        copy.start()
        receivers = places.shape[1]
        slots = lax.broadcasted_iota(jnp.int32, (receivers, receivers), 0)
        chosen = jnp.where(slots == places[...], 1.0, 0.0).T.astype(jnp.bfloat16)
        copy.wait()
        for component in range(whole.shape[0] // receivers):
            span = pl.ds(component * receivers, receivers)
            first, second = split(whole[span, :])
            high[span, :] = jnp.dot(chosen, first, preferred_element_type=jnp.float32).astype(jnp.bfloat16)
            low[span, :] = jnp.dot(chosen, second, preferred_element_type=jnp.float32).astype(jnp.bfloat16)


def ordered(gate, places, probe, before=None):
    inside = pl.BlockSpec(memory_space=VMEM)
    shape = pltpu.VMEM(probe.shape, jnp.bfloat16)
    more = () if before is None else tuple(before)
    return pl.pallas_call(
        order_kernel,
        out_shape=(shape, shape),
        in_specs=[pl.BlockSpec(memory_space=SMEM), inside, pl.BlockSpec(memory_space=HBM)] + [inside] * len(more),
        out_specs=(inside, inside),
        input_output_aliases={3 + number: number for number in range(len(more))},
        scratch_shapes=[pltpu.VMEM(probe.shape, jnp.float32), pltpu.SemaphoreType.DMA],
        compiler_params=pltpu.CompilerParams(vmem_limit_bytes=16 * 1024 * 1024),
        name="order",
    )(gate, places, probe, *more)


def gather_kernel(start, aliased, core, own, arrived, high, low, *refs):
    straight, partial_value, loaded, turned, values, in_sems, out_sems, value_sem = refs[aliased:]
    size = own.shape[0]
    half = straight.shape[1] // 2
    pieces = (own, arrived)
    sides = (core[0], 1 - core[0])
    incoming = [pltpu.make_async_copy(piece, loaded.at[number], in_sems.at[number]) for number, piece in enumerate(pieces)]
    for copy in incoming:
        copy.start()
    outgoing = []
    for number, side in enumerate(sides):
        incoming[number].wait()
        span = pl.ds(number * size, size)
        turned[:, span] = loaded[number].T
        place = pl.ds(pl.multiple_of(side * half + start, size), size)
        outgoing.append(pltpu.make_async_copy(turned.at[:, span], straight.at[:, place], out_sems.at[number]))
        outgoing[-1].start()
        first, second = split(turned[:, span])
        receivers = high.shape[0] // 2
        for component in range(2):
            rows = pl.ds(component * receivers, receivers)
            value = jnp.dot(high[rows, :], first, preferred_element_type=jnp.float32)
            value += jnp.dot(high[rows, :], second, preferred_element_type=jnp.float32)
            value += jnp.dot(low[rows, :], first, preferred_element_type=jnp.float32)
            values[:, component, :, span] = value.reshape(values.shape[0], values.shape[2], size)
    last = pltpu.make_async_copy(values, partial_value, value_sem)
    last.start()
    for copy in outgoing:
        copy.wait()
    last.wait()


def gathered(start, core, own, arrived, high, low, owners, columns, straight=None):
    size, trace = own.shape
    inside = pl.BlockSpec(memory_space=VMEM)
    anywhere = pl.BlockSpec(memory_space=HBM)
    more = () if straight is None else (straight,)
    shape = (owners, 2, high.shape[0] // (2 * owners), 2 * size)
    return pl.pallas_call(
        functools.partial(gather_kernel, start, len(more)),
        out_shape=(pltpu.HBM((trace, columns), jnp.float32), pltpu.HBM(shape, jnp.float32)),
        in_specs=[pl.BlockSpec(memory_space=SMEM), anywhere, anywhere, inside, inside] + [anywhere] * len(more),
        out_specs=(anywhere, anywhere),
        input_output_aliases={5 + number: number for number in range(len(more))},
        scratch_shapes=[
            pltpu.VMEM((2, size, trace), jnp.float32),
            pltpu.VMEM((trace, 2 * size), jnp.float32),
            pltpu.VMEM(shape, jnp.float32),
            pltpu.SemaphoreType.DMA((2,)),
            pltpu.SemaphoreType.DMA((2,)),
            pltpu.SemaphoreType.DMA,
        ],
        compiler_params=pltpu.CompilerParams(vmem_limit_bytes=18 * 1024 * 1024),
        name="gather",
    )(core, own, arrived, high, low, *more)


def local(sources, green, probe, batch_pick, owner_map):
    column = lax.axis_index("gx")
    row = lax.axis_index("gz")
    columns = lax.axis_size("gx")
    rows = lax.axis_size("gz")
    core = lax.bitwise_and(row, 1)
    chip_diag = lax.shift_right_logical(row, 1) + column
    operator = green[0, 0]
    trace = operator.shape[0]
    window = batch_pick.shape[0]
    half = window // 2
    shots = sources.shape[4]
    units = half * shots // UNIT
    steps = units + SKEW * (columns + rows // 2 - 2)
    size = half * shots // 2

    here = pltpu.with_memory_space_constraint(sources[0, 0], HBM)
    operator = pltpu.with_memory_space_constraint(operator, HBM)
    probes = pltpu.with_memory_space_constraint(probe[0, 0], HBM)
    other_operator = swapped(operator, "gz")
    on_diag = lax.dynamic_index_in_dim(batch_pick, row + column, 1, keepdims=False).reshape(2, half)
    picks = jnp.where(core == 0, on_diag, on_diag[::-1])
    core_word = core.astype(jnp.int32).reshape(1)
    places = owner_map
    late = (chip_diag < 2).astype(jnp.int32).reshape(1)
    early = 1 - late
    base = (SKEW * chip_diag).astype(jnp.int32).reshape(1)
    picks, places, late, early, core_word, base = lax.optimization_barrier((picks, places, late, early, core_word, base))
    for_other = picked(picks, here)
    pairs, inputs, store = own_side(core_word, picks, operator, here)
    theirs = swapped(for_other, "gz")
    high, low = ordered(early, places, probes)
    pairs, inputs = other_side(core_word, other_operator, theirs, pairs, inputs)

    uppers = [jnp.zeros((UNIT, trace), jnp.float32)] * SKEW
    lefters = [jnp.zeros((2, UNIT, trace), jnp.float32)] * SKEW
    for step in range(steps):
        right, lower, store = swept(step, units, base, pairs, inputs, uppers[step], lefters[step], store)
        if step + SKEW < steps:
            first = max(bound for bound in BOUNDS if bound <= step)
            after = min(bound for bound in BOUNDS if bound > step)

            def live(diag, first=first, after=after):
                return after > SKEW * diag > first - units

            lefters.append(passed_along(right, (1, 0), live))
            uppers.append(passed_along(lower, (0, 2), live))
        if step == steps - 16:
            high, low = ordered(late, places, probes, (high, low))
        if step == steps - 8:
            own_part, other_part = released(0, size, core_word, store)
            base, other_part = lax.optimization_barrier((base, other_part))
            arrived = swapped(other_part, "gz")
            straight, partial_value = gathered(0, core_word, own_part, arrived, high, low, columns, window * shots)

    own_part, other_part = released(size, size, core_word, store)
    arrived = swapped(other_part, "gz")
    first_sums = lax.all_to_all(partial_value, "gx", split_axis=0, concat_axis=0, tiled=True)
    first_sum = first_sums.sum(axis=0)
    straight, partial_value = gathered(size, core_word, own_part, arrived, high, low, columns, window * shots, straight)
    second_sum = lax.all_to_all(partial_value, "gx", split_axis=0, concat_axis=0, tiled=True).sum(axis=0)
    own_sum = jnp.concatenate([first_sum[..., :size], second_sum[..., :size]], -1)
    far_sum = jnp.concatenate([first_sum[..., size:], second_sum[..., size:]], -1)
    total = jnp.where(core == 0, jnp.concatenate([own_sum, far_sum], -1), jnp.concatenate([far_sum, own_sum], -1))
    return (straight[None, None], total[None])


def solution(mesh):
    return jax.shard_map(
        local,
        mesh=mesh,
        in_specs=(
            P("gz", "gx", None, None, None),
            P("gz", "gx", None, None),
            P("gz", "gx", None, None),
            P(),
            P("gz", None),
        ),
        out_specs=(P("gz", "gx", None, None), P("gz", None, "gx", None)),
        check_vma=False,
    )
```
